32 devices in a mesh: outer: 2 (over x), dp: 16 (over z, y, core).
Axes of the slice: x: 2, y: 2, z: 4, core: 2. Of those that a mesh axis runs over, the one named last changes fastest.
Arguments:
- fast_weights: float32 [2, 4096, 2048], P('outer', 'dp'), may hold values from -6 to 6
- slow_weights: float32 [4096, 2048], P('dp', 'outer'), may hold values from -6 to 6
- momentum: float32 [4096, 2048], P('dp', 'outer'), may hold values from -3 to 3
- tokens: bfloat16 [24576, 4096], P(('outer', 'dp')), may hold values from -6 to 6
- norm_gain: float32 [4096], replicated, may hold values from 0.1 to 1.9
Outputs:
- slow_next: float32 [4096, 2048], P('dp', 'outer')
- momentum_next: float32 [4096, 2048], P('dp', 'outer')
- fast_next: float32 [4096, 2048], P('dp')
- key_values: bfloat16 [24576, 2048], P(('outer', 'dp'))
The draws below stay inside these ranges and needn't reach their ends.
All inputs are finite; a program needn't handle non-finite values.
Results may differ from the reference program's by a relative error of at most 0.0057.
Values may be sent and summed in bfloat16 or wider, within the bound.
No kernel may reach another device: no remote copies, remote signals or barrier semaphores. Data moves between devices by JAX's collectives and lax.ppermute only.
A program may use at most 128 MiB of HBM per device.

```python
import jax
import jax.numpy as jnp
from jax import lax

D = 4096
TOK_DEV = 768
COLS = 2048
PODS = 2
TOKENS = 24576
N_OUTER = 2


def strengthened(values, stream_key, source, target, parts, factor):
    def block_of(axis_at):
        return (jnp.arange(values.shape[axis_at]) // (values.shape[axis_at] // parts)).reshape((-1,) + (1,) * (values.ndim - 1 - axis_at))

    first = jax.random.permutation(stream_key, parts)[block_of(target)]
    far = (block_of(target) + parts // 2) % parts
    return jnp.where((block_of(source) == first) | (block_of(source) == far), factor * values, values)


def steps_of(rng, shape, cuts, least, high):
    loudness = 1.0
    for axis_at, blocks in cuts:
        steps = jax.random.uniform(jax.random.fold_in(jax.random.fold_in(rng, 6), axis_at), (blocks,), jnp.float32, least / len(cuts), high / len(cuts))
        loudness = loudness * jnp.repeat(jnp.exp(steps), shape[axis_at] // blocks).reshape((-1,) + (1,) * (len(shape) - 1 - axis_at))
    return loudness


def normal_values(rng, shape, width, limit, shards=(), kind=jnp.bfloat16):
    factor_of = steps_of(rng, shape, shards, -0.22, 0.18) if shards else 1.0
    entries = jax.random.normal(rng, shape, jnp.float32) * width * factor_of
    return jnp.minimum(jnp.maximum(entries, -limit), limit).astype(kind)


def noise_with(rng, dims, width, reach, split, heavy, held_as=jnp.bfloat16):
    result = width * jax.random.normal(rng, dims, jnp.float32)
    if split:
        result = result * steps_of(rng, dims, split, -0.22, 0.18)
    return jnp.clip(strengthened(result, jax.random.fold_in(rng, 3), *heavy), -reach, reach).astype(held_as)


def setup_inputs(seed: int = 0) -> dict:
    splits = jax.random.split(jax.random.key(seed), 6)
    fast_weights = noise_with(splits[0], (PODS, D, COLS), 1.0, 6.0, ((0, 2), (1, 16)), (0, 2, 2, 2.0), jnp.float32)
    slow_weights = normal_values(splits[1], (D, COLS), 1.0, 6.0, ((0, 16), (1, 2)), jnp.float32)
    momentum = normal_values(splits[2], (D, COLS), 0.5, 3.0, ((0, 16), (1, 2)), jnp.float32)
    tokens = normal_values(splits[3], (TOKENS, D), 1.0, 6.0, ((0, 32),))
    norm_gain = jnp.clip(1.0 + 0.18 * jax.random.normal(splits[4], (D,), jnp.float32), 0.1, 1.9)
    return dict(fast_weights=fast_weights, slow_weights=slow_weights, momentum=momentum, tokens=tokens, norm_gain=norm_gain)


OUTER_LR = 0.7
MOMENTUM_COEF = 0.9
EPSILON = 1e-05

def reference(fast_weights, slow_weights, momentum, tokens, norm_gain):
    outer_grad = lax.optimization_barrier(jnp.sum(slow_weights[None] - fast_weights, axis=0)) / N_OUTER
    momentum_next = MOMENTUM_COEF * momentum + outer_grad
    slow_next = slow_weights - OUTER_LR * (outer_grad + MOMENTUM_COEF * momentum_next)
    fast_next = slow_next
    weights_rounded = slow_next.astype(jnp.bfloat16).astype(jnp.float32)
    blocks = tokens.reshape(TOKENS // TOK_DEV, TOK_DEV, D)

    def project(block):
        values = block.astype(jnp.float32)
        meansq = lax.optimization_barrier(jnp.mean(values * values, axis=-1, keepdims=True))
        normed = (values * lax.rsqrt(meansq + EPSILON) * norm_gain).astype(jnp.bfloat16)
        product = jnp.dot(normed.astype(jnp.float32), weights_rounded, preferred_element_type=jnp.float32)
        return (product * D ** (-0.5)).astype(jnp.bfloat16)
    key_values = lax.map(project, blocks).reshape(TOKENS, COLS)
    return (slow_next, momentum_next, fast_next, key_values)
```

```python
import functools

import jax
import jax.numpy as jnp
from jax import lax
from jax.experimental import pallas as pl
from jax.experimental.pallas import tpu as pltpu
from jax.sharding import PartitionSpec as P

OUTER_LR = 0.7
MOMENTUM_COEF = 0.9
EPSILON = 1e-05
LANES = 128
CORES = 2
ROWS = 2


def outer_update(slow_part, moment_part, fast_total, pod_count):
    outer_grad = slow_part - fast_total / pod_count
    moment_next = MOMENTUM_COEF * moment_part + outer_grad
    slow_next = slow_part - OUTER_LR * (outer_grad + MOMENTUM_COEF * moment_next)
    return (slow_next, moment_next)


def chunk_plan(width):
    units = width // LANES
    if units < 8:
        return (("zyx", 0, width),)
    third = 3 * units // 8 * LANES
    return (("zyx", 0, third), ("zxy", third, third), ("xyz", 2 * third, width - 2 * third))


def norm_kernel(place, tokens, gain, out, *, depth, blocks):
    values = tokens[...].astype(jnp.float32)
    meansq = jnp.mean(values * values, axis=-1, keepdims=True)
    scale = lax.rsqrt(meansq + EPSILON)
    y, c = place[0], place[1]
    at = 0
    for dc in range(CORES):
        for dy in range(ROWS):
            for z in range(blocks):
                source = (z * ROWS + jnp.bitwise_xor(y, dy)) * CORES + jnp.bitwise_xor(c, dc)
                columns = pl.ds(pl.multiple_of(source * depth, depth), depth)
                part = tokens[:, columns].astype(jnp.float32)
                out[:, at : at + depth] = (part * scale * gain[:, columns]).astype(jnp.bfloat16)
                at += depth


def normed_by_place(tokens, gain, place, depth, tile):
    rows, width = tokens.shape
    return pl.pallas_call(
        functools.partial(norm_kernel, depth=depth, blocks=width // (depth * ROWS * CORES)),
        out_shape=jax.ShapeDtypeStruct((rows, width), jnp.bfloat16),
        grid_spec=pltpu.PrefetchScalarGridSpec(
            num_scalar_prefetch=1,
            grid=(rows // tile,),
            in_specs=[
                pl.BlockSpec((tile, width), lambda i, place: (i, 0)),
                pl.BlockSpec((1, width), lambda i, place: (0, 0)),
            ],
            out_specs=pl.BlockSpec((tile, width), lambda i, place: (i, 0)),
        ),
        cost_estimate=pl.CostEstimate(flops=20 * rows * width, bytes_accessed=4 * rows * width, transcendentals=0),
        name="norm",
    )(place, tokens, gain.reshape(1, width))


def product_kernel(base, normed, *refs, scale, parts, aliased):
    weights = refs[:parts]
    out, held, sems = refs[parts + aliased :]
    step, steps = pl.program_id(0), pl.num_programs(0)
    tile, columns = held.shape[1:]
    slot = lax.rem(step, 2)

    def copy(at, which):
        rows = pl.ds(pl.multiple_of(at * tile, tile), tile)
        lanes = pl.ds(pl.multiple_of(base[0], LANES), columns)
        return pltpu.make_async_copy(held.at[which], out.at[rows, lanes], sems.at[which])

    @pl.when(step >= 2)
    def _():
        copy(step - 2, slot).wait()

    depth = normed.shape[1] // parts
    total = None
    for part, weight in enumerate(weights):
        block = weight[...].reshape(depth, columns)
        piece = jnp.dot(normed[:, part * depth : (part + 1) * depth], block, preferred_element_type=jnp.float32)
        total = piece if total is None else total + piece
    held[slot] = (total * scale).astype(held.dtype)
    copy(step, slot).start()

    @pl.when(step == steps - 1)
    def _():
        @pl.when(steps >= 2)
        def _():
            copy(step - 1, 1 - slot).wait()

        copy(step, slot).wait()


def product(normed, weights, base, out, shape, tile):
    rows, width = normed.shape
    columns = weights[0][0].shape[-1]
    specs = [pl.BlockSpec((tile, width), lambda i, base: (i, 0))]
    operands = []
    for array, index in weights:
        shape_of = (array.shape[0],) + (None,) * len(index) + array.shape[-2:]
        specs.append(pl.BlockSpec(shape_of, functools.partial(lambda i, base, index: (0,) + index + (0, 0), index=index)))
        operands.append(array)
    aliases = {}
    if out is not None:
        specs.append(pl.BlockSpec(memory_space=pl.ANY))
        operands.append(out)
        aliases = {1 + len(operands): 0}
    return pl.pallas_call(
        functools.partial(product_kernel, scale=width ** (-0.5), parts=len(weights), aliased=len(aliases)),
        out_shape=jax.ShapeDtypeStruct(shape, jnp.bfloat16),
        grid_spec=pltpu.PrefetchScalarGridSpec(
            num_scalar_prefetch=1,
            grid=(rows // tile,),
            in_specs=specs,
            out_specs=pl.BlockSpec(memory_space=pl.ANY),
            scratch_shapes=[pltpu.VMEM((2, tile, columns), jnp.bfloat16), pltpu.SemaphoreType.DMA((2,))],
        ),
        input_output_aliases=aliases,
        cost_estimate=pl.CostEstimate(
            flops=2 * rows * width * columns, bytes_accessed=2 * (rows * width + (width + rows) * columns), transcendentals=0
        ),
        name="product",
    )(base.reshape(1), normed, *operands)


def body(fast_weights, slow_weights, momentum, tokens, norm_gain):
    pods, devices = lax.axis_size("outer"), lax.axis_size("dp")
    depths = devices // (ROWS * CORES)
    x, place = lax.axis_index("outer"), lax.axis_index("dp")
    z, y, c = place // (ROWS * CORES), place // CORES % ROWS, place % CORES
    fast = fast_weights[0]
    rows, cols = fast.shape
    width = cols // pods

    def shifted(value, shift):
        return lax.ppermute(value, "outer", [(i, (i + shift) % pods) for i in range(pods)])

    def over_x(value):
        return [shifted(value, shift) for shift in range(1, pods)]

    def over_y(value):
        return lax.ppermute(value, "dp", [(i, i ^ CORES) for i in range(devices)])

    def over_core(value):
        return lax.ppermute(value, "dp", [(i, i ^ 1) for i in range(devices)])

    groups = [[i * ROWS * CORES + j for i in range(depths)] for j in range(ROWS * CORES)]

    def over_z(value):
        copies = jnp.broadcast_to(value[None], (depths,) + value.shape)
        return lax.all_to_all(copies, "dp", 0, 0, axis_index_groups=groups, tiled=True)

    chunks = chunk_plan(width)
    received = []
    for _, first, size in chunks:
        parts = []
        for shift in range(1, pods):
            at = (x + shift) % pods * width + first
            parts.append(shifted(lax.dynamic_slice(fast, (0, at), (rows, size)).astype(jnp.bfloat16), shift))
        received.append(parts)

    normed = normed_by_place(tokens, norm_gain, jnp.stack([y, c]).astype(jnp.int32), rows, min(256, tokens.shape[0]))
    gathered, mirrors = [], []
    for (order, first, size), parts in zip(chunks, received):
        total = lax.dynamic_slice(fast, (0, x * width + first), (rows, size))
        for part in parts:
            total = total + part.astype(jnp.float32)
        mine, _ = outer_update(slow_weights[:, first : first + size], momentum[:, first : first + size], total, pods)
        mine = mine.astype(jnp.bfloat16)
        if order == "xyz":
            over = [mine] + over_x(mine)
            mirrors.append(over[1:])
            pieces = jnp.stack(over)
            both = jnp.stack([pieces, over_y(pieces)], axis=1)
            spread = over_z(both)
            other = over_core(spread)
            gathered.append([[(a, (d, e)) for a in (spread, other) for e in range(ROWS)] for d in range(pods)])
        else:
            near = over_z(mine)
            if order == "zyx":
                far = over_y(near)
                near_x, far_x = over_x(near), over_x(far)
            else:
                near_x = over_x(near)
                far, far_x = over_y(near), [over_y(v) for v in near_x]
            mirrors.append([lax.dynamic_slice(v, (z, 0, 0), (1, rows, size))[0] for v in near_x])
            by_part = [(near, far)] + list(zip(near_x, far_x))
            gathered.append([[(v, ()) for v in (a, b, over_core(a), over_core(b))] for a, b in by_part])

    key_values = None
    shape = (tokens.shape[0], cols)
    for (order, first, size), by_part in zip(chunks, gathered):
        for d, weights in enumerate(by_part):
            base = ((x + pods - d) % pods * width + first).astype(jnp.int32)
            key_values = product(normed, weights, base, key_values, shape, min(256, tokens.shape[0]))

    total = lax.dynamic_slice(fast, (0, x * width), (rows, width))
    for shift in range(pods - 1):
        total = total + jnp.concatenate([parts[shift] for parts in received], axis=1).astype(jnp.float32)
    slow_next, momentum_next = outer_update(slow_weights, momentum, total, pods)
    parts = [slow_next]
    for d in range(pods - 1):
        parts.append(jnp.concatenate([m[d] for m in mirrors], axis=1).astype(jnp.float32))
    fast_next = jnp.zeros((rows, cols), jnp.float32)
    for d, part in enumerate(parts):
        fast_next = lax.dynamic_update_slice(fast_next, part, (0, (x + pods - d) % pods * width))
    return (slow_next, momentum_next, fast_next, key_values)


def solution(mesh):
    in_specs = (
        P("outer", "dp", None),
        P("dp", "outer"),
        P("dp", "outer"),
        P(("outer", "dp"), None),
        P(),
    )
    out_specs = (P("dp", "outer"), P("dp", "outer"), P("dp", None), P(("outer", "dp"), None))
    return jax.shard_map(body, mesh=mesh, in_specs=in_specs, out_specs=out_specs, check_vma=False)
```
